256 devices in a mesh: row: 16 (over y_hi, x, core), col: 16 (over z, y_lo).
Axes of the slice: x: 4, y: 4 (y_hi: 2, y_lo: 2; y = y_hi * 2 + y_lo), z: 8, core: 2. Of those that a mesh axis runs over, the one named last changes fastest.
Arguments:
- features: bfloat16 [32768, 512], P(('row', 'col')), may hold values from -6 to 6
- coefs: bfloat16 [32768], P(('row', 'col')), may hold values from -150 to 150
Outputs:
- grads: bfloat16 [32768, 512], P(('row', 'col'))
- recolored: bfloat16 [32768, 512], P(('row', 'col'))
The draws below stay inside these ranges and needn't reach their ends.
All inputs are finite; a program needn't handle non-finite values.
Results may differ from the reference program's by a relative error of at most 0.0025.
The reference program's roundings to bfloat16 on the way (of `kernel`, `weighted` and `agop`) count: a program that leaves them out, or rounds other values in their place, can miss the bound.
Values may be sent and summed in bfloat16 or wider, within the bound.
No kernel may reach another device: no remote copies, remote signals or barrier semaphores. Data moves between devices by JAX's collectives and lax.ppermute only.
A program may use at most 64 MiB of HBM per device.

```python
import jax
import jax.numpy as jnp
from jax import lax

D = 512
NPTS = 32768


def block_scale(rng, extent, pieces, smallest, largest):
    factor_of, own = 1.0, jax.random.fold_in(rng, 6)
    for axis_at, shards_of in pieces:
        steps = jnp.exp(jax.random.uniform(jax.random.fold_in(own, axis_at), (shards_of,), jnp.float32, smallest / len(pieces), largest / len(pieces)))
        factor_of = factor_of * jnp.repeat(steps, extent[axis_at] // shards_of).reshape([-1 if axis == axis_at else 1 for axis in range(len(extent))])
    return factor_of


def scatter_about(rng, extent, scale, most, shards=(), kind=jnp.bfloat16):
    gain = block_scale(rng, extent, shards, -0.22, 0.18) if shards else 1.0
    result = jax.random.normal(rng, extent, jnp.float32) * scale * gain
    return jnp.minimum(jnp.maximum(result, -most), most).astype(kind)


def setup_inputs(seed: int = 0) -> dict:
    arg_keys = jax.random.split(jax.random.key(seed), 3)
    return {
        "features": scatter_about(arg_keys[0], (NPTS, D), 1.0, 6.0, ((0, 256),)),
        "coefs": scatter_about(arg_keys[1], (NPTS,), 25.0, 150.0, ((0, 256),)),
    }


def reference(features, coefs):
    width = features.shape[1]
    gamma = 2.0 / width
    feats_full = features.astype(jnp.float32)
    coef_full = coefs.astype(jnp.float32)
    norms = jnp.sum(feats_full * feats_full, axis=1)
    weighted = (coef_full[:, None] * feats_full).astype(jnp.bfloat16)
    weighted_full = lax.optimization_barrier(weighted).astype(jnp.float32)
    strip_len = min(512, NPTS)
    strip_count = NPTS // strip_len

    def one_strip(packed):
        strip_feats, strip_norms = packed
        products = jnp.dot(strip_feats, feats_full.T, precision=lax.Precision.HIGHEST)
        kernel = jnp.exp(-(strip_norms[:, None] + norms[None, :] - 2.0 * products) * gamma).astype(jnp.bfloat16)
        kernel_full = lax.optimization_barrier(kernel).astype(jnp.float32)
        totals = jnp.dot(kernel_full, coef_full, precision=lax.Precision.HIGHEST)
        moments = jnp.dot(kernel_full, weighted_full, precision=lax.Precision.HIGHEST)
        return totals, moments

    totals, moments = lax.map(one_strip, (feats_full.reshape(strip_count, strip_len, width), norms.reshape(strip_count, strip_len)))
    totals = totals.reshape(NPTS)
    moments = moments.reshape(NPTS, width)
    grads = (2.0 * gamma * (moments - totals[:, None] * feats_full)).astype(jnp.bfloat16)
    grads_full = lax.optimization_barrier(grads).astype(jnp.float32)
    gram = jnp.dot(grads_full.T, grads_full, precision=lax.Precision.HIGHEST)
    agop = (gram / NPTS).astype(jnp.bfloat16)
    agop_full = lax.optimization_barrier(agop).astype(jnp.float32)
    recolored = jnp.dot(feats_full, agop_full, precision=lax.Precision.HIGHEST).astype(jnp.bfloat16)
    return grads, recolored
```

```python
import math

import jax
import jax.numpy as jnp
from jax import lax
from jax.experimental import pallas as pl
from jax.experimental.pallas import tpu as pltpu
from jax.sharding import Mesh, PartitionSpec as P


AXES = ("yh", "x", "c", "z", "yl")
SIZES = (2, 4, 2, 8, 2)
EXTRA = 8
LANES = 128
VMEM_LIMIT = 12 * 2**20
F32, BF16 = jnp.float32, jnp.bfloat16


def swapped(value, axis):
    return lax.ppermute(value, axis, [(0, 1), (1, 0)])


def from_everyone(value, axes):
    copies = jnp.broadcast_to(value, (lax.axis_size(axes), *value.shape))
    return lax.all_to_all(copies, axes, split_axis=0, concat_axis=0, tiled=True)


def along_z(value):
    count = lax.axis_size("z")
    pairs = [(z, (z + 1) % count) for z in range(count)]
    pairs += [(count + z, count + (z - 1) % count) for z in range(count)]
    return lax.ppermute(value, ("c", "z"), pairs)


def extra_rows(features, coefs):
    full = features.astype(F32)
    norms = jnp.sum(full * full, axis=1)
    high = lax.reduce_precision(norms, 8, 7)
    middle = lax.reduce_precision(norms - high, 8, 7)
    low = lax.reduce_precision(norms - high - middle, 8, 7)
    rows = jnp.stack([coefs.astype(F32), high, middle, low]).astype(BF16)
    return jnp.pad(rows, ((0, EXTRA - 4), (0, 0)))


def widened(rows, width):
    return jnp.pad(rows, ((0, 0), (0, width - rows.shape[1])))


def pair_block(features, coefs):
    points, width = features.shape
    extras = extra_rows(features, coefs)
    block = jnp.concatenate([features, widened(extras, width)])
    other = swapped(block, "yh")
    extras = jnp.concatenate([extras, other[points:, :points]], axis=1)
    return jnp.concatenate([features, other[:points], widened(extras, width)])


def tile_kernel(first, last, row_refs_count, chunk_count, *refs):
    row_refs, refs = refs[:row_refs_count], refs[row_refs_count:]
    chunk_refs, refs = refs[:chunk_count], refs[chunk_count:]
    if not first:
        old_ref, old_totals_ref, *refs = refs
    out_ref, refs = refs[0], refs[1:]
    if not last:
        totals_ref, refs = refs[0], refs[1:]
    (weighted_ref,) = refs
    row_count, width = row_refs[0].shape
    points = chunk_refs[0].shape[0] - EXTRA
    scale = 2.0 / width * math.log2(math.e)
    lane = lax.broadcasted_iota(jnp.int32, (LANES, LANES), 1)
    sublane = lax.broadcasted_iota(jnp.int32, (LANES, LANES), 0)
    for at, ref in enumerate(chunk_refs):
        for k in range(0, points, LANES):
            coef_row = ref[points : points + 1, k : k + LANES].astype(F32)
            spread = jnp.where(lane == sublane, coef_row, 0.0).astype(BF16)
            weighted_ref[at * points + k : at * points + k + LANES, :] = jnp.dot(
                spread, ref[k : k + LANES, :], preferred_element_type=F32
            ).astype(BF16)

    for s in range(0, row_refs_count, 2):
        strip = 2 * row_count
        here = slice(s * row_count, s * row_count + strip)
        rows = jnp.concatenate([row_refs[s][...], row_refs[s + 1][...]])
        full = rows.astype(F32)
        row_terms = jnp.sum(full * full, axis=1, keepdims=True) * (-scale)
        totals = jnp.zeros((strip, LANES), F32) if first else old_totals_ref[here, :]
        kernels = []
        for ref in chunk_refs:
            extra = ref[points : points + EXTRA, :points].astype(F32)
            col_terms = (extra[1:2] + extra[2:3] + extra[3:4]) * (-scale)
            products = lax.dot_general(
                rows, ref[:points, :], (((1,), (1,)), ((), ())), preferred_element_type=F32
            )
            kernel = jnp.exp2(products * (2.0 * scale) + (row_terms + col_terms)).astype(BF16)
            terms = kernel.astype(F32) * extra[0:1]
            for k in range(0, points, LANES):
                totals = totals + terms[:, k : k + LANES]
            kernels.append(kernel)
        moments = jnp.dot(
            jnp.concatenate(kernels, axis=1), weighted_ref[...], preferred_element_type=F32
        )
        if not first:
            moments = moments + old_ref[here, :]
        if last:
            moments = moments - jnp.sum(totals, axis=1, keepdims=True) * full
            x_at, yl_at = lax.axis_index("x"), lax.axis_index("yl")
            for k in range(0, strip, LANES):
                away, beside = divmod((here.start + k) // LANES, 2)
                place = 2 * lax.rem(x_at + away, row_refs_count) + lax.rem(yl_at + beside, 2)
                out_ref[place] = moments[k : k + LANES]
        else:
            out_ref[here, :] = moments
            totals_ref[here, :] = totals


def add_tiles(rows, chunks, carried, last):
    row_count, width = sum(r.shape[0] for r in rows), rows[0].shape[1]
    columns = sum(chunk.shape[0] - EXTRA for chunk in chunks)
    first = carried is None
    spec = pl.BlockSpec(memory_space=pltpu.VMEM)
    operands = [*rows, *chunks] + ([] if first else list(carried))
    aliases = {}
    if last:
        out_shape = [jax.ShapeDtypeStruct((row_count // LANES, LANES, width), F32)]
    else:
        out_shape = [
            jax.ShapeDtypeStruct((row_count, width), F32),
            jax.ShapeDtypeStruct((row_count, LANES), F32),
        ]
        if not first:
            aliases = {len(operands) - 2: 0, len(operands) - 1: 1}

    def body(*refs):
        tile_kernel(first, last, len(rows), len(chunks), *refs)

    return pl.pallas_call(
        body,
        out_shape=out_shape,
        in_specs=[spec] * len(operands),
        out_specs=[spec] * len(out_shape),
        scratch_shapes=[pltpu.VMEM((columns, width), BF16)],
        input_output_aliases=aliases,
        compiler_params=pltpu.CompilerParams(vmem_limit_bytes=VMEM_LIMIT),
        cost_estimate=pl.CostEstimate(
            flops=4 * row_count * columns * width,
            bytes_accessed=4 * row_count * width,
            transcendentals=row_count * columns,
        ),
    )(*operands)


def step(features, coefs):
    points, width = features.shape
    gamma = 2.0 / width
    row_axes = ("x", "yl")
    chip_axes = ("yh", "x", "z", "yl")

    beside = swapped(features, "yl")
    rows = [jnp.concatenate([features, beside])]
    x_count = lax.axis_size("x")
    for shift in range(1, x_count):
        pairs = [(x, (x - shift) % x_count) for x in range(x_count)]
        rows.append(lax.ppermute(rows[0], "x", pairs))
    near = pair_block(features, coefs)
    far = swapped(near, "c")
    groups = [[near, far]]
    hops = lax.axis_size("z") // 2
    for hop in range(1, hops + 1):
        near = along_z(near)
        other_near = swapped(near, "c")
        if hop == hops:
            groups += [[near], [other_near]]
            break
        far = along_z(far)
        other_far = swapped(far, "c")
        groups.append([near, far, other_near, other_far])

    carried = None
    for at, group in enumerate(groups):
        carried = add_tiles(rows, group, carried, at == len(groups) - 1)
    (partial,) = carried
    summed = jnp.sum(lax.all_to_all(partial, row_axes, 0, 0, tiled=True), axis=0)
    grads = (2.0 * gamma * summed).astype(BF16)

    core = lax.axis_index("c")
    half = width // 2
    both = jnp.concatenate([grads, swapped(grads, "c")])
    own_half = jnp.where(core == 0, both[:, :half], both[:, half:])
    gram = jnp.einsum("pa,pb->ab", own_half, both, preferred_element_type=F32)
    chips = lax.axis_size(chip_axes)
    parts = lax.all_to_all(gram.reshape(chips, -1, 128), chip_axes, 0, 0, tiled=True)
    point_count = points * chips * lax.axis_size("c")
    own_agop = (jnp.sum(parts, axis=0) / point_count).astype(BF16)
    own_rows = from_everyone(own_agop, chip_axes).reshape(half, width)
    other_rows = swapped(own_rows, "c")
    upper = jnp.where(core == 0, own_rows, other_rows)
    lower = jnp.where(core == 0, other_rows, own_rows)
    agop = jnp.concatenate([upper, lower])
    recolored = jnp.dot(features, agop, preferred_element_type=F32)
    return grads, recolored.astype(BF16)


def solution(mesh):
    fine = Mesh(mesh.devices.reshape(SIZES), AXES)
    return jax.shard_map(
        step,
        mesh=fine,
        in_specs=(P(AXES, None), P(AXES)),
        out_specs=(P(AXES, None), P(AXES, None)),
        check_vma=False,
    )
```

```python
import math

import jax
import jax.numpy as jnp
from jax import lax
from jax.experimental import pallas as pl
from jax.experimental.pallas import tpu as pltpu
from jax.sharding import Mesh, PartitionSpec as P


AXES = ("yh", "x", "c", "z", "yl")
SIZES = (2, 4, 2, 8, 2)
EXTRA = 8
LANES = 128
VMEM_LIMIT = 12 * 2**20
F32, BF16 = jnp.float32, jnp.bfloat16


def swapped(value, axis):
    return lax.ppermute(value, axis, [(0, 1), (1, 0)])


def from_everyone(value, axes):
    copies = jnp.broadcast_to(value, (lax.axis_size(axes), *value.shape))
    return lax.all_to_all(copies, axes, split_axis=0, concat_axis=0, tiled=True)


def along_z(value):
    count = lax.axis_size("z")
    pairs = [(z, (z + 1) % count) for z in range(count)]
    pairs += [(count + z, count + (z - 1) % count) for z in range(count)]
    return lax.ppermute(value, ("c", "z"), pairs)


def beside_y(value):
    pairs = []
    for yh in range(2):
        for c in range(2):
            for yl in range(2):
                pairs.append(((yh * 2 + c) * 2 + yl, ((yh ^ c) * 2 + c) * 2 + 1 - yl))
    return lax.ppermute(value, ("yh", "c", "yl"), pairs)


def in_vmem(body, out_shape, *operands, **params):
    spec = pl.BlockSpec(memory_space=pltpu.VMEM)
    several = isinstance(out_shape, list)
    return pl.pallas_call(
        body,
        out_shape=out_shape,
        in_specs=[spec] * len(operands),
        out_specs=[spec] * len(out_shape) if several else spec,
        compiler_params=pltpu.CompilerParams(vmem_limit_bytes=VMEM_LIMIT),
        **params,
    )(*operands)


def pack_kernel(features_ref, coefs_ref, out_ref):
    points, width = features_ref.shape
    features = features_ref[...]
    full = features.astype(F32)
    square = full * full
    high = square.astype(BF16)
    low = (square - high.astype(F32)).astype(BF16)
    ones = jnp.ones((EXTRA, width), BF16)
    norms = sum(
        lax.dot_general(ones, part, (((1,), (1,)), ((), ())), preferred_element_type=F32)
        for part in (high, low)
    )
    pieces, rest = [coefs_ref[...].astype(F32)], norms
    for _ in range(3):
        pieces.append(rest.astype(BF16).astype(F32))
        rest = rest - pieces[-1]
    row = lax.broadcasted_iota(jnp.int32, (EXTRA, points), 0)
    extra = jnp.zeros((EXTRA, points), F32)
    for at, piece in enumerate(pieces):
        extra = jnp.where(row == at, piece, extra)
    out_ref[:points, :] = features
    out_ref[points:, :] = jnp.zeros((EXTRA, width), BF16)
    out_ref[points:, :points] = extra.astype(BF16)


def pair_kernel(near_ref, other_ref, out_ref):
    width = near_ref.shape[1]
    points = near_ref.shape[0] - EXTRA
    out_ref[2 * points :, :] = jnp.zeros((EXTRA, width), BF16)
    for at, ref in enumerate((near_ref, other_ref)):
        here = slice(at * points, (at + 1) * points)
        out_ref[here, :] = ref[:points, :]
        out_ref[2 * points :, here] = ref[points:, :points]


def pair_block(features, coefs):
    points, width = features.shape
    shape = jax.ShapeDtypeStruct((points + EXTRA, width), BF16)
    block = in_vmem(pack_kernel, shape, features, coefs.reshape(1, -1))
    other = swapped(block, "yh")
    shape = jax.ShapeDtypeStruct((2 * points + EXTRA, width), BF16)
    return in_vmem(pair_kernel, shape, block, other)


def recolor_kernel(features_ref, own_ref, other_ref, out_ref):
    half = own_ref.shape[0]
    core = lax.axis_index("c")

    def store(upper_ref, lower_ref):
        out = jnp.dot(features_ref[:, :half], upper_ref[...], preferred_element_type=F32)
        out = out + jnp.dot(features_ref[:, half:], lower_ref[...], preferred_element_type=F32)
        out_ref[...] = out.astype(BF16)

    @pl.when(core == 0)
    def _():
        store(own_ref, other_ref)

    @pl.when(core != 0)
    def _():
        store(other_ref, own_ref)


def tile_kernel(first, sides, row_refs_count, chunk_count, *refs):
    last = len(sides) == 1
    row_refs, refs = refs[:row_refs_count], refs[row_refs_count:]
    chunk_refs, refs = refs[:chunk_count], refs[chunk_count:]
    if not first:
        old_ref, old_totals_ref, *refs = refs
    if last:
        out_refs, refs = refs[:row_refs_count], refs[row_refs_count:]
    else:
        out_ref, totals_ref, *refs = refs
    (weighted_ref,) = refs
    row_count, width = row_refs[0].shape
    points = chunk_refs[0].shape[0] - EXTRA
    scale = 2.0 / width * math.log2(math.e)
    lane = lax.broadcasted_iota(jnp.int32, (LANES, LANES), 1)
    sublane = lax.broadcasted_iota(jnp.int32, (LANES, LANES), 0)
    for at, ref in enumerate(chunk_refs):
        for k in range(0, points, LANES):
            coef_row = ref[points : points + 1, k : k + LANES].astype(F32)
            spread = jnp.where(lane == sublane, coef_row, 0.0).astype(BF16)
            weighted_ref[at * points + k : at * points + k + LANES, :] = jnp.dot(
                spread, ref[k : k + LANES, :], preferred_element_type=F32
            ).astype(BF16)

    shard = row_count // 2
    strip = row_refs_count * shard
    for side in sides:
        here = slice(side * strip, (side + 1) * strip)
        rows = jnp.concatenate([ref[side * shard : (side + 1) * shard] for ref in row_refs])
        full = rows.astype(F32)
        row_terms = jnp.sum(full * full, axis=1, keepdims=True) * (-scale)
        totals = jnp.zeros((strip, LANES), F32) if first else old_totals_ref[here, :]
        kernels = []
        for ref in chunk_refs:
            extra = ref[points : points + EXTRA, :points].astype(F32)
            col_terms = (extra[1:2] + extra[2:3] + extra[3:4]) * (-scale)
            products = lax.dot_general(
                rows, ref[:points, :], (((1,), (1,)), ((), ())), preferred_element_type=F32
            )
            kernel = jnp.exp2(products * (2.0 * scale) + (row_terms + col_terms)).astype(BF16)
            terms = kernel.astype(F32) * extra[0:1]
            for k in range(0, points, LANES):
                totals = totals + terms[:, k : k + LANES]
            kernels.append(kernel)
        moments = jnp.dot(
            jnp.concatenate(kernels, axis=1), weighted_ref[...], preferred_element_type=F32
        )
        if not first:
            moments = moments + old_ref[here, :]
        if last:
            moments = moments - jnp.sum(totals, axis=1, keepdims=True) * full
            for at, ref in enumerate(out_refs):
                ref[...] = moments[at * shard : (at + 1) * shard]
        else:
            out_ref[here, :] = moments
            totals_ref[here, :] = totals


def add_tiles(rows, chunks, carried, sides=(0, 1)):
    width = rows[0].shape[1]
    row_count = sum(r.shape[0] for r in rows) * len(sides) // 2
    columns = sum(chunk.shape[0] - EXTRA for chunk in chunks)
    first, last = carried is None, len(sides) == 1
    operands = [*rows, *chunks] + ([] if first else list(carried))
    aliases = {}
    if last:
        out_shape = [jax.ShapeDtypeStruct((row_count // len(rows), width), F32)] * len(rows)
    else:
        out_shape = [
            jax.ShapeDtypeStruct((row_count, width), F32),
            jax.ShapeDtypeStruct((row_count, LANES), F32),
        ]
        if not first:
            aliases = {len(operands) - 2: 0, len(operands) - 1: 1}

    def body(*refs):
        tile_kernel(first, sides, len(rows), len(chunks), *refs)

    return in_vmem(
        body,
        out_shape,
        *operands,
        scratch_shapes=[pltpu.VMEM((columns, width), BF16)],
        input_output_aliases=aliases,
        cost_estimate=pl.CostEstimate(
            flops=4 * row_count * columns * width,
            bytes_accessed=4 * row_count * width,
            transcendentals=row_count * columns,
        ),
    )


def summed_partials(own, beside):
    count = len(own)
    totals = [None] * count
    parts = []
    for at in ((2, 1), (3, 0)):
        parts.append((at, beside_y(jnp.stack([beside[k] for k in at]))))
    for at, part in parts:
        for i, k in enumerate(at):
            totals[k] = own[k] + part[i]
    result = totals[0]
    for k in (2, 1, 3):
        pairs = [(x, (x + k) % count) for x in range(count)]
        result = result + lax.ppermute(totals[k], "x", pairs)
    return result


def step(features, coefs):
    points, width = features.shape
    gamma = 2.0 / width
    chip_axes = ("yh", "x", "z", "yl")

    beside = beside_y(features)
    rows = [jnp.concatenate([features, beside])]
    x_count = lax.axis_size("x")
    for shift in range(1, x_count):
        pairs = [(x, (x - shift) % x_count) for x in range(x_count)]
        rows.append(lax.ppermute(rows[0], "x", pairs))
    near = pair_block(features, coefs)
    far = swapped(near, "c")
    groups = [[near, far]]
    hops = lax.axis_size("z") // 2
    for hop in range(1, hops + 1):
        near = along_z(near)
        other_near = swapped(near, "c")
        if hop == hops:
            groups += [[near], [other_near]]
            break
        far = along_z(far)
        other_far = swapped(far, "c")
        groups.append([near, far, other_near, other_far])

    carried = None
    for group in groups[:-1]:
        carried = add_tiles(rows, group, carried)
    beside = add_tiles(rows, groups[-1], carried, sides=(1,))
    own = add_tiles(rows, groups[-1], carried, sides=(0,))
    grads = (2.0 * gamma * summed_partials(own, beside)).astype(BF16)

    core = lax.axis_index("c")
    half = width // 2
    both = jnp.concatenate([grads, swapped(grads, "c")])
    own_half = jnp.where(core == 0, both[:, :half], both[:, half:])
    gram = jnp.einsum("pa,pb->ab", own_half, both, preferred_element_type=F32)
    chips = lax.axis_size(chip_axes)
    parts = lax.all_to_all(gram.reshape(chips, -1, 128), chip_axes, 0, 0, tiled=True)
    point_count = points * chips * lax.axis_size("c")
    own_agop = (jnp.sum(parts, axis=0) / point_count).astype(BF16)
    own_rows = from_everyone(own_agop, chip_axes).reshape(half, width)
    other_rows = swapped(own_rows, "c")
    recolored = in_vmem(
        recolor_kernel, jax.ShapeDtypeStruct((points, width), BF16), features, own_rows, other_rows
    )
    return grads, recolored


def solution(mesh):
    fine = Mesh(mesh.devices.reshape(SIZES), AXES)
    return jax.shard_map(
        step,
        mesh=fine,
        in_specs=(P(AXES, None), P(AXES)),
        out_specs=(P(AXES, None), P(AXES, None)),
        check_vma=False,
    )
```

```python
import math

import jax
import jax.numpy as jnp
from jax import lax
from jax.experimental import pallas as pl
from jax.experimental.pallas import tpu as pltpu
from jax.sharding import Mesh, PartitionSpec as P


AXES = ("yh", "x", "c", "z", "yl")
SIZES = (2, 4, 2, 8, 2)
EXTRA = 8
LANES = 128
VMEM_LIMIT = 12 * 2**20
F32, BF16 = jnp.float32, jnp.bfloat16


def swapped(value, axis):
    return lax.ppermute(value, axis, [(0, 1), (1, 0)])


def from_everyone(value, axes):
    copies = jnp.broadcast_to(value, (lax.axis_size(axes), *value.shape))
    return lax.all_to_all(copies, axes, split_axis=0, concat_axis=0, tiled=True)


def along_z(value):
    count = lax.axis_size("z")
    pairs = [(z, (z + 1) % count) for z in range(count)]
    pairs += [(count + z, count + (z - 1) % count) for z in range(count)]
    return lax.ppermute(value, ("c", "z"), pairs)


def beside_y(value):
    pairs = []
    for yh in range(2):
        for c in range(2):
            for yl in range(2):
                pairs.append(((yh * 2 + c) * 2 + yl, ((yh ^ c) * 2 + c) * 2 + 1 - yl))
    return lax.ppermute(value, ("yh", "c", "yl"), pairs)


def in_vmem(body, out_shape, *operands, **params):
    spec = pl.BlockSpec(memory_space=pltpu.VMEM)
    several = isinstance(out_shape, list)
    return pl.pallas_call(
        body,
        out_shape=out_shape,
        in_specs=[spec] * len(operands),
        out_specs=[spec] * len(out_shape) if several else spec,
        compiler_params=pltpu.CompilerParams(vmem_limit_bytes=VMEM_LIMIT),
        **params,
    )(*operands)


def pack_kernel(features_ref, coefs_ref, out_ref):
    points, width = features_ref.shape
    features = features_ref[...]
    full = features.astype(F32)
    square = full * full
    high = square.astype(BF16)
    low = (square - high.astype(F32)).astype(BF16)
    ones = jnp.ones((EXTRA, width), BF16)
    norms = sum(
        lax.dot_general(ones, part, (((1,), (1,)), ((), ())), preferred_element_type=F32)
        for part in (high, low)
    )
    pieces, rest = [coefs_ref[...].astype(F32)], norms
    for _ in range(3):
        pieces.append(rest.astype(BF16).astype(F32))
        rest = rest - pieces[-1]
    row = lax.broadcasted_iota(jnp.int32, (EXTRA, points), 0)
    extra = jnp.zeros((EXTRA, points), F32)
    for at, piece in enumerate(pieces):
        extra = jnp.where(row == at, piece, extra)
    out_ref[:points, :] = features
    out_ref[points:, :] = jnp.zeros((EXTRA, width), BF16)
    out_ref[points:, :points] = extra.astype(BF16)


def pair_kernel(near_ref, other_ref, out_ref):
    width = near_ref.shape[1]
    points = near_ref.shape[0] - EXTRA
    out_ref[2 * points :, :] = jnp.zeros((EXTRA, width), BF16)
    for at, ref in enumerate((near_ref, other_ref)):
        here = slice(at * points, (at + 1) * points)
        out_ref[here, :] = ref[:points, :]
        out_ref[2 * points :, here] = ref[points:, :points]


def pair_block(features, coefs):
    points, width = features.shape
    shape = jax.ShapeDtypeStruct((points + EXTRA, width), BF16)
    block = in_vmem(pack_kernel, shape, features, coefs.reshape(1, -1))
    other = swapped(block, "yh")
    shape = jax.ShapeDtypeStruct((2 * points + EXTRA, width), BF16)
    return in_vmem(pair_kernel, shape, block, other)


def recolor_kernel(features_ref, own_ref, other_ref, out_ref):
    half = own_ref.shape[0]
    core = lax.axis_index("c")

    def store(upper_ref, lower_ref):
        out = jnp.dot(features_ref[:, :half], upper_ref[...], preferred_element_type=F32)
        out = out + jnp.dot(features_ref[:, half:], lower_ref[...], preferred_element_type=F32)
        out_ref[...] = out.astype(BF16)

    @pl.when(core == 0)
    def _():
        store(own_ref, other_ref)

    @pl.when(core != 0)
    def _():
        store(other_ref, own_ref)


def tile_kernel(first, last, sides, row_refs_count, chunk_count, *refs):
    row_refs, refs = refs[:row_refs_count], refs[row_refs_count:]
    chunk_refs, refs = refs[:chunk_count], refs[chunk_count:]
    if not first:
        old_ref, old_totals_ref, *refs = refs
    if last:
        out_refs, refs = refs[:row_refs_count], refs[row_refs_count:]
    else:
        out_ref, totals_ref, *refs = refs
    (weighted_ref,) = refs
    row_count, width = row_refs[0].shape
    points = chunk_refs[0].shape[0] - EXTRA
    scale = 2.0 / width * math.log2(math.e)
    lane = lax.broadcasted_iota(jnp.int32, (LANES, LANES), 1)
    sublane = lax.broadcasted_iota(jnp.int32, (LANES, LANES), 0)
    for at, ref in enumerate(chunk_refs):
        for k in range(0, points, LANES):
            coef_row = ref[points : points + 1, k : k + LANES].astype(F32)
            spread = jnp.where(lane == sublane, coef_row, 0.0).astype(BF16)
            weighted_ref[at * points + k : at * points + k + LANES, :] = jnp.dot(
                spread, ref[k : k + LANES, :], preferred_element_type=F32
            ).astype(BF16)

    shard = row_count // 2
    strip = row_refs_count * shard
    for side in sides:
        here = slice(side * strip, (side + 1) * strip)
        rows = jnp.concatenate([ref[side * shard : (side + 1) * shard] for ref in row_refs])
        full = rows.astype(F32)
        row_terms = jnp.sum(full * full, axis=1, keepdims=True) * (-scale)
        totals = jnp.zeros((strip, LANES), F32) if first else old_totals_ref[here, :]
        kernels = []
        for ref in chunk_refs:
            extra = ref[points : points + EXTRA, :points].astype(F32)
            col_terms = (extra[1:2] + extra[2:3] + extra[3:4]) * (-scale)
            products = lax.dot_general(
                rows, ref[:points, :], (((1,), (1,)), ((), ())), preferred_element_type=F32
            )
            kernel = jnp.exp2(products * (2.0 * scale) + (row_terms + col_terms)).astype(BF16)
            terms = kernel.astype(F32) * extra[0:1]
            for k in range(0, points, LANES):
                totals = totals + terms[:, k : k + LANES]
            kernels.append(kernel)
        moments = jnp.dot(
            jnp.concatenate(kernels, axis=1), weighted_ref[...], preferred_element_type=F32
        )
        if not first:
            moments = moments + old_ref[here, :]
        if last:
            moments = moments - jnp.sum(totals, axis=1, keepdims=True) * full
            for at, ref in enumerate(out_refs):
                ref[...] = moments[at * shard : (at + 1) * shard]
        else:
            out_ref[here, :] = moments
            totals_ref[here, :] = totals


def add_tiles(rows, chunks, carried, sides=(0, 1), last=False):
    width = rows[0].shape[1]
    row_count = sum(r.shape[0] for r in rows)
    columns = sum(chunk.shape[0] - EXTRA for chunk in chunks)
    first = carried is None
    operands = [*rows, *chunks] + ([] if first else list(carried))
    aliases = {}
    if last:
        shard = row_count // len(rows) // 2
        out_shape = [jax.ShapeDtypeStruct((shard, width), F32)] * len(rows)
    else:
        out_shape = [
            jax.ShapeDtypeStruct((row_count, width), F32),
            jax.ShapeDtypeStruct((row_count, LANES), F32),
        ]
        if not first:
            aliases = {len(operands) - 2: 0, len(operands) - 1: 1}

    done = row_count * len(sides) // 2

    def body(*refs):
        tile_kernel(first, last, sides, len(rows), len(chunks), *refs)

    return in_vmem(
        body,
        out_shape,
        *operands,
        scratch_shapes=[pltpu.VMEM((columns, width), BF16)],
        input_output_aliases=aliases,
        cost_estimate=pl.CostEstimate(
            flops=4 * done * columns * width,
            bytes_accessed=4 * done * width,
            transcendentals=done * columns,
        ),
    )


def summed_partials(own, beside):
    count = len(own)
    onward = [(x, (x + 1) % count) for x in range(count)]
    back = [(x, (x - 1) % count) for x in range(count)]
    half = own[0].shape[0] // 2
    far = beside_y(beside[2])
    sides = beside_y(jnp.stack([beside[1], beside[3]]))
    near = beside_y(beside[0])
    far = own[2] + far
    up = lax.ppermute(far[:half], "x", onward)
    down = lax.ppermute(far[half:], "x", back)
    sums = [own[1] + sides[0], own[3] + sides[1]]
    sums[0] = sums[0] + jnp.pad(up, ((0, half), (0, 0)))
    sums[1] = sums[1] + jnp.pad(down, ((half, 0), (0, 0)))
    from_below = lax.ppermute(sums[0], "x", onward)
    from_above = lax.ppermute(sums[1], "x", back)
    return own[0] + near + from_below + from_above


def step(features, coefs):
    points, width = features.shape
    gamma = 2.0 / width
    chip_axes = ("yh", "x", "z", "yl")

    beside = beside_y(features)
    rows = [jnp.concatenate([features, beside])]
    x_count = lax.axis_size("x")
    for shift in range(1, x_count):
        pairs = [(x, (x - shift) % x_count) for x in range(x_count)]
        rows.append(lax.ppermute(rows[0], "x", pairs))
    near = pair_block(features, coefs)
    far = swapped(near, "c")
    groups = [[near, far]]
    hops = lax.axis_size("z") // 2
    for hop in range(1, hops + 1):
        near = along_z(near)
        other_near = swapped(near, "c")
        if hop == hops:
            groups += [[near], [other_near]]
            break
        far = along_z(far)
        other_far = swapped(far, "c")
        groups.append([near, far, other_near, other_far])

    carried, waiting = None, groups[-3] + groups[-2] + groups[-1]
    for at, group in enumerate(groups[:-2]):
        carried = add_tiles(rows, group, carried, (1,) if at == hops - 1 else (0, 1))
    beside = add_tiles(rows, groups[-2] + groups[-1], carried, (1,), last=True)
    own = add_tiles(rows, waiting, carried, (0,), last=True)
    grads = (2.0 * gamma * summed_partials(own, beside)).astype(BF16)

    core = lax.axis_index("c")
    half = width // 2
    both = jnp.concatenate([grads, swapped(grads, "c")])
    own_half = jnp.where(core == 0, both[:, :half], both[:, half:])
    gram = jnp.einsum("pa,pb->ab", own_half, both, preferred_element_type=F32)
    chips = lax.axis_size(chip_axes)
    parts = lax.all_to_all(
        gram.astype(BF16).reshape(chips, -1, LANES), chip_axes, 0, 0, tiled=True
    ).astype(F32)
    point_count = points * chips * lax.axis_size("c")
    own_agop = (jnp.sum(parts, axis=0) / point_count).astype(BF16)
    own_rows = from_everyone(own_agop, chip_axes).reshape(half, width)
    other_rows = swapped(own_rows, "c")
    recolored = in_vmem(
        recolor_kernel, jax.ShapeDtypeStruct((points, width), BF16), features, own_rows, other_rows
    )
    return grads, recolored


def solution(mesh):
    fine = Mesh(mesh.devices.reshape(SIZES), AXES)
    return jax.shard_map(
        step,
        mesh=fine,
        in_specs=(P(AXES, None), P(AXES)),
        out_specs=(P(AXES, None), P(AXES, None)),
        check_vma=False,
    )
```
